32 devices in a mesh: batch: 4 (over x, core), lat: 8 (over z, y).
Axes of the slice: x: 2, y: 2, z: 4, core: 2. Of those that a mesh axis runs over, the one named last changes fastest.
Arguments:
- predicted: bfloat16 [4, 73, 192, 1440], P('batch', None, 'lat'), may hold values from -64 to 64
- target: bfloat16 [4, 73, 192, 1440], P('batch', None, 'lat'), may hold values from -128 to 128
- legendre_basis: bfloat16 [192, 96, 720], P(None, ('batch', 'lat')), may hold values from -1 to 1
Outputs:
- spectra: float32 [2, 73, 720], replicated
- channel_loss: float32 [73], replicated
The draws below stay inside these ranges and needn't reach their ends.
All inputs are finite; a program needn't handle non-finite values.
Results may differ from the reference program's by a relative error of at most 0.0003.
Values may be sent and summed in bfloat16 or wider, within the bound.
A program may use at most 128 MiB of HBM per device.

```python
import math
import jax
import jax.numpy as jnp
from jax import lax

C = 73
NLON = 1440
L = 720
NLAT = 192
BATCH = 4
M = 96


def channel_scales(key):
    base_key = jax.random.fold_in(key, 7001)
    logs = jax.random.uniform(base_key, (C,), jnp.float32, 0.0, 0.6)
    return jnp.exp(logs)


def target_factors(key):
    ratio_key = jax.random.fold_in(key, 7002)
    return jnp.exp(jax.random.uniform(ratio_key, (C,), jnp.float32, -0.7, 0.7))


def field_entries(key, shape):
    return jnp.clip(jax.random.normal(key, shape, jnp.float32), -6.0, 6.0)


def draw_predicted(key, part):
    scales = channel_scales(key)
    values = field_entries(jax.random.fold_in(key, 7003), (BATCH, C, NLAT, NLON))
    return (values * scales[None, :, None, None]).astype(jnp.bfloat16)


def draw_target(key, part):
    scales = channel_scales(key) * target_factors(key)
    values = field_entries(jax.random.fold_in(key, 7004), (BATCH, C, NLAT, NLON))
    return (values * scales[None, :, None, None]).astype(jnp.bfloat16)


def draw_legendre_basis(key, part):
    values = field_entries(jax.random.fold_in(key, 7005), (NLAT, M, L))
    scaled = jnp.clip(values / jnp.sqrt(jnp.float32(NLAT)), -1.0, 1.0)
    return scaled.astype(jnp.bfloat16)


def setup_inputs(seed: int = 0) -> dict:
    splits = jax.random.split(jax.random.key(seed), 4)
    return {
        "predicted": draw_predicted(jax.random.fold_in(splits[3], 71), 0),
        "target": draw_target(jax.random.fold_in(splits[3], 71), 0),
        "legendre_basis": draw_legendre_basis(jax.random.fold_in(splits[3], 71), 0),
    }


def fourier_table():
    lon_ids = jnp.arange(NLON, dtype=jnp.int32)
    order_ids = jnp.arange(M, dtype=jnp.int32)
    product_ids = lon_ids[:, None] * order_ids[None, :] % NLON
    angles = 2.0 * math.pi / NLON * product_ids.astype(jnp.float32)
    inv_root = 1.0 / math.sqrt(NLON)
    return jnp.stack([jnp.cos(angles) * inv_root, -jnp.sin(angles) * inv_root], axis=1).astype(jnp.bfloat16)

def reference(predicted, target, legendre_basis):
    dft_table = fourier_table().astype(jnp.float32)
    basis_wide = legendre_basis.astype(jnp.float32)
    order_ids = jnp.arange(M, dtype=jnp.int32)
    weights = jnp.where(order_ids == 0, 1.0, 2.0).astype(jnp.float32)

    def member_energy(field_in):
        fourier = jnp.einsum('cnk,kpm->pmcn', field_in.astype(jnp.float32), dft_table).astype(jnp.bfloat16)
        coefficients = jnp.einsum('pmcn,nml->pmcl', fourier.astype(jnp.float32), basis_wide)
        squares = lax.optimization_barrier(jnp.sum(coefficients * coefficients, axis=0))
        return lax.optimization_barrier(jnp.sum(squares * weights[:, None, None], axis=0))
    energy_pred = lax.optimization_barrier(jnp.sum(lax.map(member_energy, predicted), axis=0))
    energy_target = lax.optimization_barrier(jnp.sum(lax.map(member_energy, target), axis=0))
    spectra = jnp.stack([energy_pred, energy_target], axis=0) / (BATCH * M)
    log_spectra = jnp.log(spectra + 1e-06)
    channel_loss = lax.optimization_barrier(jnp.mean((log_spectra[0] - log_spectra[1]) ** 2, axis=1))
    return (spectra, channel_loss)
```

```python
import functools
import math

import jax
import jax.numpy as jnp
import numpy as np
from jax import lax
from jax.experimental import pallas as pl
from jax.experimental.pallas import tpu as pltpu
from jax.sharding import PartitionSpec as P

MESH = pl.DeviceIdType.MESH
VMEM_SPEC = pl.BlockSpec(memory_space=pltpu.VMEM)


def fourier_table(lon_count, order_count):
    product_ids = np.arange(lon_count)[:, None] * np.arange(order_count)[None, :] % lon_count
    angles = np.float32(2.0 * math.pi / lon_count) * product_ids.astype(np.float32)
    inv_root = np.float32(1.0 / math.sqrt(lon_count))
    table = np.stack([np.cos(angles) * inv_root, -np.sin(angles) * inv_root], axis=2)
    return table.astype(jnp.bfloat16)


def greet_all(groups, bands):
    count = groups * bands
    me = lax.axis_index("batch") * bands + lax.axis_index("lat")
    barrier = pltpu.get_barrier_semaphore()

    @pl.loop(1, count)
    def _(step):
        peer = lax.rem(me + step, count)
        pl.semaphore_signal(
            barrier, inc=1, device_id=(peer // bands, lax.rem(peer, bands)), device_id_type=MESH
        )

    pl.semaphore_wait(barrier, count - 1)


def exchange_kernel(groups, bands, send_ref, recv_ref, send_sem, recv_sem):
    count = groups * bands
    me = lax.axis_index("batch") * bands + lax.axis_index("lat")
    greet_all(groups, bands)

    def copy_to(peer, slot):
        return pltpu.make_async_remote_copy(
            src_ref=send_ref.at[peer],
            dst_ref=recv_ref.at[slot],
            send_sem=send_sem.at[peer],
            recv_sem=recv_sem.at[slot],
            device_id=(peer // bands, lax.rem(peer, bands)),
            device_id_type=MESH,
        )

    @pl.loop(1, count)
    def _(step):
        copy_to(lax.rem(me + step, count), me).start()

    recv_ref[me] = send_ref[me]

    @pl.loop(1, count)
    def _(step):
        peer = lax.rem(me + step, count)
        copy_to(peer, peer).wait_recv()
        copy_to(peer, peer).wait_send()


def exchange(groups, bands, blocks):
    count = groups * bands
    return pl.pallas_call(
        functools.partial(exchange_kernel, groups, bands),
        out_shape=jax.ShapeDtypeStruct(blocks.shape, blocks.dtype),
        in_specs=[VMEM_SPEC],
        out_specs=VMEM_SPEC,
        scratch_shapes=[pltpu.SemaphoreType.DMA((count,)), pltpu.SemaphoreType.DMA((count,))],
        compiler_params=pltpu.CompilerParams(collective_id=0, has_side_effects=True),
    )(blocks)


def total_kernel(groups, bands, part_ref, out_ref, first, second, mid, sems):
    my_group = lax.axis_index("batch")
    my_band = lax.axis_index("lat")
    greet_all(groups, bands)

    def over(axis_size, mine, make):
        @pl.loop(1, axis_size)
        def _(step):
            make(lax.rem(mine + step, axis_size), mine).start()

    def finish(axis_size, mine, make):
        @pl.loop(1, axis_size)
        def _(step):
            peer = lax.rem(mine + step, axis_size)
            make(peer, peer).wait_recv()
            make(peer, peer).wait_send()

    def scatter_groups(peer, slot):
        return pltpu.make_async_remote_copy(
            src_ref=part_ref.at[peer], dst_ref=first.at[slot],
            send_sem=sems.at[0, peer], recv_sem=sems.at[1, slot],
            device_id=(peer, my_band), device_id_type=MESH,
        )

    def scatter_bands(peer, slot):
        return pltpu.make_async_remote_copy(
            src_ref=mid.at[peer], dst_ref=second.at[slot],
            send_sem=sems.at[2, peer], recv_sem=sems.at[3, slot],
            device_id=(my_group, peer), device_id_type=MESH,
        )

    def gather_bands(peer, slot):
        return pltpu.make_async_remote_copy(
            src_ref=out_ref.at[my_group, my_band], dst_ref=out_ref.at[my_group, slot],
            send_sem=sems.at[4, peer], recv_sem=sems.at[5, slot],
            device_id=(my_group, peer), device_id_type=MESH,
        )

    def gather_groups(peer, slot):
        return pltpu.make_async_remote_copy(
            src_ref=out_ref.at[my_group], dst_ref=out_ref.at[slot],
            send_sem=sems.at[6, peer], recv_sem=sems.at[7, slot],
            device_id=(peer, my_band), device_id_type=MESH,
        )

    over(groups, my_group, scatter_groups)
    first[my_group] = part_ref[my_group]
    finish(groups, my_group, scatter_groups)
    mid[...] = jnp.sum(first[...], axis=0)

    over(bands, my_band, scatter_bands)
    second[my_band] = mid[my_band]
    finish(bands, my_band, scatter_bands)
    out_ref[my_group, my_band] = jnp.sum(second[...], axis=0)

    over(bands, my_band, gather_bands)
    finish(bands, my_band, gather_bands)
    over(groups, my_group, gather_groups)
    finish(groups, my_group, gather_groups)


def total(groups, bands, part):
    widest = max(groups, bands)
    tile = part.shape[2:]
    return pl.pallas_call(
        functools.partial(total_kernel, groups, bands),
        out_shape=jax.ShapeDtypeStruct(part.shape, part.dtype),
        in_specs=[VMEM_SPEC],
        out_specs=VMEM_SPEC,
        scratch_shapes=[
            pltpu.VMEM((groups, bands) + tile, jnp.float32),
            pltpu.VMEM((bands,) + tile, jnp.float32),
            pltpu.VMEM((bands,) + tile, jnp.float32),
            pltpu.SemaphoreType.DMA((8, widest)),
        ],
        compiler_params=pltpu.CompilerParams(collective_id=1, has_side_effects=True),
    )(part)


def body(predicted, target, legendre_basis):
    groups = lax.axis_size("batch")
    bands = lax.axis_size("lat")
    count = groups * bands
    lat_total, per_dev, degrees = legendre_basis.shape
    members, channels, lat_rows, lon_count = predicted.shape
    order_count = per_dev * count
    table = jnp.asarray(fourier_table(lon_count, order_count))
    table = table.reshape(lon_count, count, per_dev, 2)

    def transform(field_in):
        return jnp.einsum(
            "bcnk,kdmp->dmpbnc", field_in, table, preferred_element_type=jnp.float32
        ).astype(jnp.bfloat16)

    blocks = jnp.stack([transform(predicted), transform(target)], axis=2)
    blocks = blocks.transpose(0, 4, 5, 1, 2, 3, 6).reshape(count, members * lat_rows, -1)
    arrived = exchange(groups, bands, blocks)
    arrived = arrived.reshape(groups, bands, members, lat_rows, per_dev, 2, 2, channels)
    basis = legendre_basis.reshape(bands, lat_rows, per_dev, degrees)
    coefficients = jnp.einsum(
        "gtbnmfpc,tnml->mgbpfcl", arrived, basis, preferred_element_type=jnp.float32
    )
    me = lax.axis_index("batch") * bands + lax.axis_index("lat")
    orders = me * per_dev + jnp.arange(per_dev, dtype=jnp.int32)
    weights = jnp.where(orders == 0, 1.0, 2.0).astype(jnp.float32)
    weights = weights[:, None, None, None, None, None, None]
    part = jnp.sum(coefficients * coefficients * weights, axis=(0, 1, 2, 3))

    rows = 2 * channels
    row_tiles, lane_tiles = -(-rows // 8), -(-degrees // 128)
    tiles = row_tiles * lane_tiles
    per_chunk = -(-tiles // count)
    part = jnp.pad(
        part.reshape(rows, degrees), ((0, row_tiles * 8 - rows), (0, lane_tiles * 128 - degrees))
    )
    part = part.reshape(row_tiles, 8, lane_tiles, 128).transpose(0, 2, 1, 3)
    part = jnp.pad(part.reshape(tiles, 8, 128), ((0, per_chunk * count - tiles), (0, 0), (0, 0)))
    energy = total(groups, bands, part.reshape(groups, bands, per_chunk, 8, 128))
    energy = energy.reshape(per_chunk * count, 8, 128)[:tiles]
    energy = energy.reshape(row_tiles, lane_tiles, 8, 128).transpose(0, 2, 1, 3)
    energy = energy.reshape(row_tiles * 8, lane_tiles * 128)[:rows, :degrees]
    energy = energy.reshape(2, channels, degrees)

    spectra = energy / (members * groups * order_count)
    log_spectra = jnp.log(spectra + 1e-06)
    channel_loss = jnp.mean((log_spectra[0] - log_spectra[1]) ** 2, axis=1)
    return (spectra, channel_loss)


def solution(mesh):
    placed = (
        P("batch", None, "lat", None),
        P("batch", None, "lat", None),
        P(None, ("batch", "lat"), None),
    )
    return jax.shard_map(body, mesh=mesh, in_specs=placed, out_specs=(P(), P()), check_vma=False)
```

```python
import functools
import math

import jax
import jax.numpy as jnp
import numpy as np
from jax import lax
from jax.experimental import pallas as pl
from jax.experimental.pallas import tpu as pltpu
from jax.sharding import PartitionSpec as P

MESH = pl.DeviceIdType.MESH
VMEM_SPEC = pl.BlockSpec(memory_space=pltpu.VMEM)


def fourier_table(lon_count, order_count):
    product_ids = np.arange(lon_count)[:, None] * np.arange(order_count)[None, :] % lon_count
    angles = np.float32(2.0 * math.pi / lon_count) * product_ids.astype(np.float32)
    inv_root = np.float32(1.0 / math.sqrt(lon_count))
    table = np.stack([np.cos(angles) * inv_root, -np.sin(angles) * inv_root], axis=2)
    return table.astype(jnp.bfloat16)


def greet_all(groups, bands):
    count = groups * bands
    me = lax.axis_index("batch") * bands + lax.axis_index("lat")
    barrier = pltpu.get_barrier_semaphore()

    @pl.loop(1, count)
    def _(step):
        peer = lax.rem(me + step, count)
        pl.semaphore_signal(
            barrier, inc=1, device_id=(peer // bands, lax.rem(peer, bands)), device_id_type=MESH
        )

    pl.semaphore_wait(barrier, count - 1)


def fused_kernel(groups, bands, scale, send_ref, basis_ref, spectra_ref, loss_ref,
                 arrived, powers, part, landed, other, pieces, send_sem, recv_sem, sums_sem, pair_sem):
    count = groups * bands
    my_group = lax.axis_index("batch")
    my_band = lax.axis_index("lat")
    me = my_group * bands + my_band
    per_dev, lat_total, degrees = basis_ref.shape
    lat_rows = lat_total // bands
    members = send_ref.shape[1] // lat_rows
    channels = spectra_ref.shape[1]
    width = 4 * channels
    greet_all(groups, bands)

    def device(peer):
        return (peer // bands, lax.rem(peer, bands))

    def block_copy(peer, slot):
        return pltpu.make_async_remote_copy(
            src_ref=send_ref.at[peer], dst_ref=arrived.at[slot],
            send_sem=send_sem.at[peer], recv_sem=recv_sem.at[slot],
            device_id=device(peer), device_id_type=MESH,
        )

    @pl.loop(1, count)
    def _(step):
        block_copy(lax.rem(me + step, count), me).start()

    arrived[me] = send_ref[me]
    powers[...] = jnp.zeros_like(powers)

    @pl.loop(1, groups + 1)
    def _(step):
        group = lax.rem(my_group + groups - step, groups)

        @pl.loop(0, bands)
        def _(band):
            source = group * bands + band

            @pl.when(source != me)
            def _():
                block_copy(source, source).wait_recv()

        for order in range(per_dev):
            start = order * width // 128 * 128
            stop = min(start + powers.shape[1], arrived.shape[2])
            weight = jnp.where(me * per_dev + order == 0, 1.0, 2.0).astype(jnp.float32)
            for member in range(members):
                rows = pl.ds(member * lat_rows, lat_rows)
                bands_in = [
                    arrived[group * bands + band, rows, start:stop].astype(jnp.float32)
                    for band in range(bands)
                ]
                fourier = jnp.concatenate(bands_in, axis=0).T.astype(jnp.bfloat16)
                coefficients = jnp.dot(
                    fourier, basis_ref[order], preferred_element_type=jnp.float32
                )
                powers[order, 0 : stop - start, 0:degrees] += weight * (coefficients * coefficients)

    row_tiles = -(-channels // 8)
    lane_tiles = powers.shape[2] // 128
    for field in range(2):
        for row in range(row_tiles):
            first = row * 8
            taken = min(8, channels - first)
            strip = jnp.zeros((taken, powers.shape[2]), jnp.float32)
            for order in range(per_dev):
                offset = order * width % 128 + field * 2 * channels + first
                for piece in range(2):
                    strip += powers[order, offset + piece * channels : offset + piece * channels + taken, :]
            for lane in range(lane_tiles):
                part[field, row * lane_tiles + lane, 0:taken, :] = strip[:, lane * 128 : (lane + 1) * 128]

    half = lax.rem(my_group, 2)
    mate = my_group + 1 - 2 * half
    pair = pltpu.make_async_remote_copy(
        src_ref=part.at[1 - half], dst_ref=landed,
        send_sem=pair_sem.at[0], recv_sem=pair_sem.at[1],
        device_id=(mate, my_band), device_id_type=MESH,
    )
    pair.start()
    pair.wait()
    part[half] = part[half] + landed[...]

    ranks = groups // 2 * bands
    rank = my_group // 2 * bands + my_band
    per_rank = part.shape[1] // ranks

    def tiles(owner):
        return pl.ds(owner * per_rank, per_rank)

    def rank_device(peer):
        return (peer // bands * 2 + half, lax.rem(peer, bands))

    def scatter(peer, slot):
        return pltpu.make_async_remote_copy(
            src_ref=part.at[half, tiles(peer)], dst_ref=pieces.at[slot],
            send_sem=sums_sem.at[0, peer], recv_sem=sums_sem.at[1, slot],
            device_id=rank_device(peer), device_id_type=MESH,
        )

    def gather(peer, slot):
        return pltpu.make_async_remote_copy(
            src_ref=landed.at[tiles(rank)], dst_ref=landed.at[tiles(slot)],
            send_sem=sums_sem.at[2, peer], recv_sem=sums_sem.at[3, slot],
            device_id=rank_device(peer), device_id_type=MESH,
        )

    def start_all(make):
        @pl.loop(1, ranks)
        def _(step):
            make(lax.rem(rank + step, ranks), rank).start()

    def wait_all(make):
        @pl.loop(1, ranks)
        def _(step):
            peer = lax.rem(rank + step, ranks)
            make(peer, peer).wait_recv()
            make(peer, peer).wait_send()

    start_all(scatter)
    pieces[rank] = part[half, tiles(rank)]
    wait_all(scatter)
    landed[tiles(rank)] = jnp.sum(pieces[...], axis=0)
    start_all(gather)
    wait_all(gather)

    last = pltpu.make_async_remote_copy(
        src_ref=landed, dst_ref=other,
        send_sem=pair_sem.at[2], recv_sem=pair_sem.at[3],
        device_id=(mate, my_band), device_id_type=MESH,
    )
    last.start()
    last.wait()
    part[half] = landed[...]
    part[1 - half] = other[...]

    for row in range(row_tiles):
        first = row * 8
        taken = min(8, channels - first)
        logs = []
        for field in range(2):
            strip = jnp.concatenate(
                [part[field, row * lane_tiles + lane] for lane in range(lane_tiles)], axis=1
            )
            strip = strip[0:taken, 0:degrees] * scale
            spectra_ref[field, first : first + taken, :] = strip
            logs.append(jnp.log(strip + 1e-06))
        gap = logs[0] - logs[1]
        loss_ref[first : first + taken, :] = jnp.sum(gap * gap, axis=1, keepdims=True) / degrees

    @pl.loop(1, count)
    def _(step):
        peer = lax.rem(me + step, count)
        block_copy(peer, peer).wait_send()


def fused(groups, bands, scale, channels, blocks, basis):
    count = groups * bands
    ranks = groups // 2 * bands
    degrees = basis.shape[2]
    lanes = -(-degrees // 128) * 128
    tiles = -(-channels // 8) * (lanes // 128)
    per_rank = -(-tiles // ranks)
    window = -(-(4 * channels + 127) // 128) * 128
    return pl.pallas_call(
        functools.partial(fused_kernel, groups, bands, scale),
        out_shape=(
            jax.ShapeDtypeStruct((2, channels, degrees), jnp.float32),
            jax.ShapeDtypeStruct((channels, 1), jnp.float32),
        ),
        in_specs=[VMEM_SPEC, VMEM_SPEC],
        out_specs=(VMEM_SPEC, VMEM_SPEC),
        scratch_shapes=[
            pltpu.VMEM(blocks.shape, blocks.dtype),
            pltpu.VMEM((basis.shape[0], window, lanes), jnp.float32),
            pltpu.VMEM((2, per_rank * ranks, 8, 128), jnp.float32),
            pltpu.VMEM((per_rank * ranks, 8, 128), jnp.float32),
            pltpu.VMEM((per_rank * ranks, 8, 128), jnp.float32),
            pltpu.VMEM((ranks, per_rank, 8, 128), jnp.float32),
            pltpu.SemaphoreType.DMA((count,)),
            pltpu.SemaphoreType.DMA((count,)),
            pltpu.SemaphoreType.DMA((4, ranks)),
            pltpu.SemaphoreType.DMA((4,)),
        ],
        compiler_params=pltpu.CompilerParams(
            collective_id=0, has_side_effects=True, vmem_limit_bytes=60 * 1024 * 1024
        ),
    )(blocks, basis)


def body(predicted, target, legendre_basis):
    groups = lax.axis_size("batch")
    bands = lax.axis_size("lat")
    count = groups * bands
    per_dev = legendre_basis.shape[1]
    members, channels, lat_rows, lon_count = predicted.shape
    order_count = per_dev * count
    table = jnp.asarray(fourier_table(lon_count, order_count))
    table = table.reshape(lon_count, count, per_dev, 2)

    def transform(field_in):
        return jnp.einsum(
            "bcnk,kdmp->dmpbnc", field_in, table, preferred_element_type=jnp.float32
        ).astype(jnp.bfloat16)

    blocks = jnp.stack([transform(predicted), transform(target)], axis=2)
    blocks = blocks.transpose(0, 4, 5, 1, 2, 3, 6).reshape(count, members * lat_rows, -1)
    scale = 1.0 / (members * groups * order_count)
    spectra, loss = fused(
        groups, bands, scale, channels, blocks, legendre_basis.transpose(1, 0, 2)
    )
    return (spectra, loss.reshape(channels))


def solution(mesh):
    placed = (
        P("batch", None, "lat", None),
        P("batch", None, "lat", None),
        P(None, ("batch", "lat"), None),
    )
    return jax.shard_map(body, mesh=mesh, in_specs=placed, out_specs=(P(), P()), check_vma=False)
```
